32 devices in a mesh: fsdp: 4 (over y, core), sp: 8 (over z, x).
Axes of the slice: x: 2, y: 2, z: 4, core: 2. Of those that a mesh axis runs over, the one named last changes fastest.
Arguments:
- hidden: bfloat16 [4, 2048, 5120], P('fsdp', 'sp'), may hold values from -6 to 6
- queries: bfloat16 [4, 2048, 4096], P('fsdp', 'sp'), may hold values from -240 to 240
- norm_gain: float32 [5120], replicated, may hold values from 0.5 to 1.5
- kv_weight: bfloat16 [5120, 2048], P('fsdp'), may hold values from -0.078125 to 0.078125
- value_bias: float32 [1024], replicated, may hold values from -3 to 3
- doc_lengths: int32 [4, 16], P('fsdp'), may hold values from 1 to 512, 2048 in all within a row
Outputs:
- attended: bfloat16 [4, 2048, 4096], P('fsdp', 'sp')
The draws below stay inside these ranges and needn't reach their ends.
Inputs may be any that keep to these rules, and one draw needn't show every extreme that they name: `doc_lengths`: each row sums to 2048 and its largest entry is 512.
All inputs are finite; a program needn't handle non-finite values.
Results may differ from the reference program's by a relative error of at most 0.0067.
Values may be sent and summed in bfloat16 or wider, within the bound.
A program may use at most 128 MiB of HBM per device.

```python
import math
import jax
import jax.numpy as jnp
import numpy as np
from jax import lax

D = 5120
QH = 32
KVH = 8
HD = 128
NDOC = 16
GROUPS = 4
SEQ = 2048
MOST = 512


def draw_queries(key, part):
    drawn = jnp.clip(jax.random.normal(key, (GROUPS, SEQ, QH * HD), jnp.float32), -6.0, 6.0)
    return drawn.astype(jnp.bfloat16)


def steps_of(rng, extent, shards, low, high):
    loudness, own = 1.0, jax.random.fold_in(rng, 6)
    for position, parts in shards:
        steps = jnp.exp(jax.random.uniform(jax.random.fold_in(own, position), (parts,), jnp.float32, low / len(shards), high / len(shards)))
        loudness = loudness * jnp.repeat(steps, extent[position] // parts).reshape([-1 if axis == position else 1 for axis in range(len(extent))])
    return loudness


def split_up(number_of, total, bound, lean):
    portions = [(1 << 20) // math.isqrt(standing ** lean) + 1 for standing in range(2, number_of + 1)]
    spare, given = total - bound - (number_of - 1), [1] * (number_of - 1)
    while spare > 0:
        movable = [i for i in range(number_of - 1) if given[i] < bound]
        whole, remaining = sum([portions[i] for i in movable]), spare
        for i in movable:
            addition = min(bound - given[i], max(1, remaining * portions[i] // whole), spare)
            given[i] = given[i] + addition
            spare = spare - addition
    return np.array([bound] + given)


def uneven(key, count, total, reach, skew):
    if count == 2:
        one = jax.random.randint(key, (), max(1, total - reach), min(reach, total - 1) + 1)
        return jnp.stack([one, total - one])
    sizes = jnp.asarray(split_up(count, total, reach, skew), jnp.int32)
    couples = (count - 1) // 2
    donor, taker = sizes[1:1 + 2 * couples:2], sizes[2:2 + 2 * couples:2]
    room = jnp.minimum(donor - 1, reach - taker)
    shifted = jax.random.randint(jax.random.fold_in(key, 1), (couples,), 0, 1 << 20) % (room + 1)
    sizes = sizes.at[1:1 + 2 * couples:2].set(donor - shifted).at[2:2 + 2 * couples:2].set(taker + shifted)
    return sizes[jax.random.permutation(jax.random.fold_in(key, 2), count)]


def gaussian(key, shape, width, most, cuts=(), kind=jnp.bfloat16):
    values = jax.random.normal(key, shape, jnp.float32) * width
    if len(cuts) > 0:
        values = steps_of(key, shape, cuts, -0.22, 0.18) * values
    return jnp.clip(values, min=-most, max=most).astype(kind)


def setup_inputs(seed: int = 0) -> dict:
    seeds = jax.random.split(jax.random.key(seed), 7)
    hidden = gaussian(seeds[0], (GROUPS, SEQ, D), 1.0, 6.0, ((0, 4), (1, 8)))
    queries = draw_queries(jax.random.fold_in(seeds[6], 71), 0)
    norm_gain = jnp.clip(1.0 + 0.1 * jax.random.normal(seeds[2], (D,), jnp.float32), 0.5, 1.5)
    kv_weight = gaussian(seeds[3], (D, 2 * KVH * HD), D ** -0.5, 0.078125, ((0, 4),))
    value_bias = gaussian(seeds[4], (KVH * HD,), 0.5, 3.0, (), jnp.float32)
    doc_lengths = jax.vmap(lambda own: uneven(own, NDOC, SEQ, MOST, 2))(jax.random.split(seeds[5], GROUPS)).reshape((GROUPS, NDOC)).astype(jnp.int32)
    return {"hidden": hidden, "queries": queries, "norm_gain": norm_gain, "kv_weight": kv_weight, "value_bias": value_bias, "doc_lengths": doc_lengths}


EPS = 1e-06

def attend(query_all, key_all, value_all, doc_ids):
    length = query_all.shape[0]
    block = min(512, length)
    longest = length // 4
    window = min(length, block + longest)
    scale = HD ** (-0.5)

    def one_block(index):
        first = (index * block).astype(jnp.int32)
        start = jnp.clip(first - longest, 0, length - window).astype(jnp.int32)
        query_block = lax.dynamic_slice_in_dim(query_all, first, block, 0).astype(jnp.float32)
        key_block = lax.dynamic_slice_in_dim(key_all, start, window, 0).astype(jnp.float32)
        value_block = lax.dynamic_slice_in_dim(value_all, start, window, 0).astype(jnp.float32)
        query_ids = lax.dynamic_slice_in_dim(doc_ids, first, block, 0)
        key_ids = lax.dynamic_slice_in_dim(doc_ids, start, window, 0)
        query_pos = first + jnp.arange(block, dtype=jnp.int32)
        key_pos = start + jnp.arange(window, dtype=jnp.int32)
        allowed = (key_pos[None, :] <= query_pos[:, None]) & (key_ids[None, :] == query_ids[:, None])
        scores = jnp.einsum('qnd,knd->nqk', query_block, key_block) * scale
        scores = jnp.where(allowed[None], scores, -jnp.inf)
        highest = lax.optimization_barrier(jnp.max(scores, axis=-1, keepdims=True))
        probs = jnp.exp(scores - highest)
        probs = (probs / lax.optimization_barrier(jnp.sum(probs, axis=-1, keepdims=True))).astype(jnp.bfloat16)
        output = jnp.einsum('nqk,knd->qnd', probs.astype(jnp.float32), value_block)
        return output.astype(jnp.bfloat16)
    blocks = lax.map(one_block, jnp.arange(length // block, dtype=jnp.int32))
    return blocks.reshape(length, query_all.shape[1], query_all.shape[2])

def reference(hidden, queries, norm_gain, kv_weight, value_bias, doc_lengths):
    wide = hidden.astype(jnp.float32)
    normed = (wide * lax.rsqrt(lax.optimization_barrier(jnp.mean(wide * wide, axis=-1, keepdims=True)) + EPS) * norm_gain).astype(jnp.bfloat16)
    projected = jnp.dot(normed.reshape(GROUPS * SEQ, D), kv_weight, preferred_element_type=jnp.float32)
    projected = projected.reshape(GROUPS, SEQ, 2 * KVH * HD)
    keys = projected[..., :KVH * HD].astype(jnp.bfloat16)
    values = (projected[..., KVH * HD:] + value_bias).astype(jnp.bfloat16)
    ratio = QH // KVH

    def one_group(operands):
        query_group, key_group, value_group, lengths = operands
        ends = jnp.cumsum(lengths).astype(jnp.int32)
        positions = jnp.arange(SEQ, dtype=jnp.int32)
        doc_ids = lax.optimization_barrier(jnp.sum((positions[:, None] >= ends[None, :]).astype(jnp.int32), axis=1)).astype(jnp.int32)
        query_heads = query_group.reshape(SEQ, QH, HD)
        key_heads = jnp.repeat(key_group.reshape(SEQ, KVH, HD), ratio, axis=1)
        value_heads = jnp.repeat(value_group.reshape(SEQ, KVH, HD), ratio, axis=1)
        return attend(query_heads, key_heads, value_heads, doc_ids).reshape(SEQ, QH * HD)
    return lax.map(one_group, (queries, keys, values, doc_lengths))
```

```python
import functools
import math

import jax
import jax.numpy as jnp
from jax import lax
from jax.experimental import pallas as pl
from jax.experimental.pallas import tpu as pltpu
from jax.sharding import PartitionSpec as P

QH = 32
KVH = 8
HD = 128
EPS = 1e-06
PAIR = 2 * HD
CHUNKS = KVH // 2
MSGS = 2 * CHUNKS
XCH = 4
QB = 128
MASKED = -1e30


def kernel(
    n, s, reach,
    x_hbm, q_hbm, gain_hbm, w_hbm, vbias_hbm, docs,
    out,
    x, q, gain, vbias, w, xs, xr, own, ps, pr, kv, mask,
    local_sem, x_sem, wsem, xsend, xrecv, psend, precv, ssend, srecv, fsend,
):
    tokens, depth = x.shape
    chips = n // 2
    rows = w_hbm.shape[0]
    half = 2 * rows
    mine = lax.axis_index("fsdp")
    i = lax.axis_index("sp")
    core = lax.rem(mine, 2)
    chip = mine // 2
    mate = chip * 2 + (1 - core)
    step = tokens // XCH

    barrier = pltpu.get_barrier_semaphore()
    pl.semaphore_signal(barrier, inc=1, device_id={"fsdp": mate})
    for o in range(1, chips):
        peer = lax.rem(chip + o, chips) * 2 + core
        pl.semaphore_signal(barrier, inc=1, device_id={"fsdp": peer})
    for b in range(1, reach + 1):
        @pl.when(i >= b)
        def _():
            pl.semaphore_signal(barrier, inc=1, device_id={"sp": i - b})

        @pl.when(i + b < s)
        def _():
            pl.semaphore_signal(barrier, inc=1, device_id={"sp": i + b})

    def xcopy(c):
        part = pl.ds(c * step, step)
        return pltpu.make_async_copy(x_hbm.at[part], x.at[part], x_sem.at[c])

    gcopy = pltpu.make_async_copy(gain_hbm, gain, local_sem.at[0])
    gcopy.start()
    for c in range(XCH):
        xcopy(c).start()
    wcopy = pltpu.make_async_copy(w_hbm, w.at[core], local_sem.at[1])
    wcopy.start()
    qcopy = pltpu.make_async_copy(q_hbm, q, local_sem.at[2])
    qcopy.start()
    bcopy = pltpu.make_async_copy(vbias_hbm, vbias, local_sem.at[3])
    bcopy.start()

    def wsend():
        return pltpu.make_async_remote_copy(
            w_hbm, w.at[core], wsem.at[0], wsem.at[1], device_id={"fsdp": mate}
        )

    def xsendcopy(o, c):
        target = lax.rem(chip + o, chips)
        part = pl.ds(c * step, step)
        return pltpu.make_async_remote_copy(
            xs.at[target, part], xr.at[o - 1, part], xsend.at[o - 1, c], xrecv.at[o - 1, c],
            device_id={"fsdp": target * 2 + core},
        )

    gcopy.wait()
    for c in range(XCH):
        xcopy(c).wait()
        part = slice(c * step, (c + 1) * step)
        wide = x[part, :].astype(jnp.float32)
        inv = lax.rsqrt(jnp.mean(wide * wide, axis=-1, keepdims=True) + EPS)
        for t in range(chips):
            piece = x[part, t * half:(t + 1) * half].astype(jnp.float32)
            piece = piece * inv * gain[:, t * half:(t + 1) * half]
            xs[t, part, :] = piece.astype(jnp.bfloat16)
        if c == 0:
            near = jnp.minimum(i, reach) + jnp.minimum(s - 1 - i, reach)
            pl.semaphore_wait(barrier, chips + near)
        for o in range(1, chips):
            xsendcopy(o, c).start()
        if c == 0:
            wsend().start()

    first = i * tokens
    width = reach * tokens + QB
    for u in range(tokens // QB):
        pos = first + u * QB + lax.broadcasted_iota(jnp.int32, (QB, 1), 0)
        start = jnp.zeros((QB, 1), jnp.int32)
        end = jnp.int32(0)
        for d in range(docs.shape[1]):
            end = end + docs[0, d]
            start = jnp.where(pos >= end, end, start)
        key = first + u * QB - reach * tokens + lax.broadcasted_iota(jnp.int32, (QB, width), 1)
        mask[u] = jnp.where((key >= start) & (key <= pos), 0.0, MASKED)
    for b in range(1, reach + 1):
        @pl.when(i < b)
        def _():
            kv[:, (reach - b) * tokens:(reach - b + 1) * tokens, :] = jnp.zeros(
                (MSGS, tokens, PAIR), jnp.bfloat16
            )

    def columns(m):
        return pl.multiple_of(lax.rem(m, 2) * (KVH * HD) + (m // 2) * PAIR, PAIR)

    def project(left, m):
        cols = pl.ds(columns(m), PAIR)
        total = jnp.dot(left[:, :rows], w[0, :, cols], preferred_element_type=jnp.float32)
        return total + jnp.dot(
            left[:, rows:], w[1, :, cols], preferred_element_type=jnp.float32
        )

    wcopy.wait()
    wsend().wait()
    bcopy.wait()
    qcopy.wait()

    @pl.loop(0, MSGS)
    def _(m):
        shift = vbias[:, pl.ds(pl.multiple_of((m // 2) * PAIR, PAIR), PAIR)]
        shift = shift * lax.rem(m, 2).astype(jnp.float32)
        own[m] = project(xs.at[chip], m) + shift

    def psendcopy(o, m):
        source = lax.rem(chip + chips - o, chips)
        return pltpu.make_async_remote_copy(
            ps.at[o - 1, m], pr.at[o - 1, m], psend.at[o - 1, m], precv.at[o - 1, m],
            device_id={"fsdp": source * 2 + core},
        )

    for o in range(1, chips):
        for c in range(XCH):
            xsendcopy(o, c).wait_recv()

    @pl.loop(0, MSGS)
    def _(m):
        for o in range(1, chips):
            ps[o - 1, m] = project(xr.at[o - 1], m).astype(jnp.bfloat16)
            psendcopy(o, m).start()

    def slot(b):
        return pl.ds((reach - b) * tokens, tokens)

    def shiftcopy(b, m):
        return pltpu.make_async_remote_copy(
            kv.at[m, slot(0)], kv.at[m, slot(b)], ssend.at[b - 1, m], srecv.at[b - 1, m],
            device_id={"sp": i + b},
        )

    def relay(m):
        return pltpu.make_async_remote_copy(
            kv.at[m, slot(2)], kv.at[m, slot(1)], fsend.at[m], srecv.at[0, m],
            device_id={"sp": i - 1},
        )

    odd = lax.rem(i, 2) == 1

    def sends(b):
        return (i + b < s) & jnp.logical_not(odd) if b == 1 else i + b < s

    def finish(m):
        total = own[m]
        for o in range(1, chips):
            psendcopy(o, m).wait_recv()
            total = total + pr[o - 1, m].astype(jnp.float32)
        kv[m, reach * tokens:, :] = total.astype(jnp.bfloat16)
        for b in range(reach, 0, -1):
            @pl.when(sends(b))
            def _():
                shiftcopy(b, m).start()

    def pass_on(m):
        @pl.when(i >= 2)
        def _():
            shiftcopy(2, m).wait_recv()

        @pl.when(odd & (i >= 3))
        def _():
            relay(m).start()

    def arrive(m):
        for b in range(1, reach + 1):
            if b != 2:
                @pl.when(i >= b)
                def _():
                    shiftcopy(b, m).wait_recv()

    factor = HD ** (-0.5) * math.log2(math.e)
    ratio = QH // KVH

    def attend(j):
        for h in range(2):
            for u in range(tokens // QB):
                base = pl.multiple_of((2 * j + h) * ratio * HD, HD)
                left = jnp.concatenate(
                    [q[u * QB:(u + 1) * QB, pl.ds(base + r * HD, HD)] for r in range(ratio)], 0
                )
                keys = kv[2 * j, u * QB:u * QB + width, h * HD:(h + 1) * HD]
                values = kv[2 * j + 1, u * QB:u * QB + width, h * HD:(h + 1) * HD]
                scores = lax.dot_general(
                    left, keys, (((1,), (1,)), ((), ())), preferred_element_type=jnp.float32
                )
                scores = scores.reshape(ratio, QB, width) + mask[u][None]
                scores = scores.reshape(ratio * QB, width)
                highest = jnp.max(scores, axis=-1, keepdims=True)
                probs = jnp.exp2((scores - highest) * factor)
                total = jnp.sum(probs, axis=-1, keepdims=True)
                result = jnp.dot(
                    probs.astype(jnp.bfloat16), values, preferred_element_type=jnp.float32
                )
                result = (result / total).astype(jnp.bfloat16)
                for r in range(ratio):
                    out[u * QB:(u + 1) * QB, pl.ds(base + r * HD, HD)] = result[
                        r * QB:(r + 1) * QB
                    ]

    @pl.loop(0, CHUNKS + 2)
    def _(t):
        @pl.when(t < CHUNKS)
        def _():
            finish(2 * t)
            finish(2 * t + 1)

        @pl.when((t >= 1) & (t < CHUNKS + 1))
        def _():
            pass_on(2 * t - 2)
            pass_on(2 * t - 1)

        @pl.when(t >= 2)
        def _():
            arrive(2 * t - 4)
            arrive(2 * t - 3)
            attend(t - 2)

    for o in range(1, chips):
        for c in range(XCH):
            xsendcopy(o, c).wait_send()

    @pl.loop(0, MSGS)
    def _(m):
        for o in range(1, chips):
            psendcopy(o, m).wait_send()
        for b in range(1, reach + 1):
            @pl.when(sends(b))
            def _():
                shiftcopy(b, m).wait_send()

        @pl.when(odd & (i >= 3))
        def _():
            relay(m).wait_send()


def shards(n, s, hidden, queries, norm_gain, kv_weight, value_bias, doc_lengths):
    _, tokens, depth = hidden.shape
    reach = s // 4
    chips = n // 2
    rows = kv_weight.shape[0]
    far = chips - 1
    vmem = pltpu.VMEM
    dma = pltpu.SemaphoreType.DMA
    anywhere = pl.BlockSpec(memory_space=pl.ANY)
    result = pl.pallas_call(
        functools.partial(kernel, n, s, reach),
        out_shape=jax.ShapeDtypeStruct((tokens, QH * HD), jnp.bfloat16),
        in_specs=[anywhere] * 5 + [pl.BlockSpec(memory_space=pltpu.SMEM)],
        out_specs=pl.BlockSpec(memory_space=pltpu.VMEM),
        scratch_shapes=[
            vmem((tokens, depth), jnp.bfloat16),
            vmem((tokens, QH * HD), jnp.bfloat16),
            vmem((1, depth), jnp.float32),
            vmem((1, KVH * HD), jnp.float32),
            vmem((2, rows, 2 * KVH * HD), jnp.bfloat16),
            vmem((chips, tokens, 2 * rows), jnp.bfloat16),
            vmem((far, tokens, 2 * rows), jnp.bfloat16),
            vmem((MSGS, tokens, PAIR), jnp.float32),
            vmem((far, MSGS, tokens, PAIR), jnp.bfloat16),
            vmem((far, MSGS, tokens, PAIR), jnp.bfloat16),
            vmem((MSGS, (reach + 1) * tokens, PAIR), jnp.bfloat16),
            vmem((tokens // QB, QB, reach * tokens + QB), jnp.float32),
            dma((4,)),
            dma((XCH,)),
            dma((2,)),
            dma((far, XCH)),
            dma((far, XCH)),
            dma((far, MSGS)),
            dma((far, MSGS)),
            dma((reach, MSGS)),
            dma((reach, MSGS)),
            dma((MSGS,)),
        ],
        compiler_params=pltpu.CompilerParams(
            collective_id=0, has_side_effects=True, vmem_limit_bytes=60 * 1024 * 1024
        ),
    )(
        hidden[0], queries[0], norm_gain.reshape(1, depth), kv_weight,
        value_bias.reshape(1, KVH * HD), doc_lengths,
    )
    return result.reshape(1, tokens, QH * HD)


def solution(mesh):
    in_specs = (
        P("fsdp", "sp", None),
        P("fsdp", "sp", None),
        P(),
        P("fsdp", None),
        P(),
        P("fsdp", None),
    )
    body = functools.partial(shards, mesh.shape["fsdp"], mesh.shape["sp"])
    return jax.shard_map(
        body, mesh=mesh, in_specs=in_specs, out_specs=P("fsdp", "sp", None), check_vma=False
    )
```

```python
import functools
import math

import jax
import jax.numpy as jnp
from jax import lax
from jax.experimental import pallas as pl
from jax.experimental.pallas import tpu as pltpu
from jax.sharding import PartitionSpec as P

QH = 32
KVH = 8
HD = 128
EPS = 1e-06
PAIR = 2 * HD
PAIRS = KVH // 2
MSGS = 2 * KVH
XCH = 8
QB = 128
MASKED = -1e30


def kernel(
    n, s, reach,
    x_hbm, q_hbm, gain_hbm, w_hbm, vbias_hbm, docs,
    out,
    x, q, gain, vbias, w, xs, xr, own, ps, pr, kv, mask,
    local_sem, x_sem, wsem, xsend, xrecv, psend, precv, ssend, srecv, fsend,
):
    tokens, depth = x.shape
    chips = n // 2
    rows = w_hbm.shape[0]
    half = 2 * rows
    mine = lax.axis_index("fsdp")
    i = lax.axis_index("sp")
    core = lax.rem(mine, 2)
    chip = mine // 2
    mate = chip * 2 + (1 - core)
    step = tokens // XCH

    barrier = pltpu.get_barrier_semaphore()
    pl.semaphore_signal(barrier, inc=1, device_id={"fsdp": mate})
    for o in range(1, chips):
        peer = lax.rem(chip + o, chips) * 2 + core
        pl.semaphore_signal(barrier, inc=1, device_id={"fsdp": peer})
    for b in range(1, reach + 1):
        @pl.when(i >= b)
        def _():
            pl.semaphore_signal(barrier, inc=1, device_id={"sp": i - b})

        @pl.when(i + b < s)
        def _():
            pl.semaphore_signal(barrier, inc=1, device_id={"sp": i + b})

    def xcopy(c):
        part = pl.ds(c * step, step)
        return pltpu.make_async_copy(x_hbm.at[part], x.at[part], x_sem.at[c])

    gcopy = pltpu.make_async_copy(gain_hbm, gain, local_sem.at[0])
    gcopy.start()
    for c in range(XCH):
        xcopy(c).start()
    wcopy = pltpu.make_async_copy(w_hbm, w.at[core], local_sem.at[1])
    qcopy = pltpu.make_async_copy(q_hbm, q, local_sem.at[2])
    bcopy = pltpu.make_async_copy(vbias_hbm, vbias, local_sem.at[3])

    def wsend():
        return pltpu.make_async_remote_copy(
            w_hbm, w.at[core], wsem.at[0], wsem.at[1], device_id={"fsdp": mate}
        )

    def xsendcopy(o, c):
        target = lax.rem(chip + o, chips)
        part = pl.ds(c * step, step)
        return pltpu.make_async_remote_copy(
            xs.at[target, part], xr.at[o - 1, part], xsend.at[o - 1, c], xrecv.at[o - 1, c],
            device_id={"fsdp": target * 2 + core},
        )

    gcopy.wait()
    for c in range(XCH):
        xcopy(c).wait()
        part = slice(c * step, (c + 1) * step)
        wide = x[part, :].astype(jnp.float32)
        inv = lax.rsqrt(jnp.mean(wide * wide, axis=-1, keepdims=True) + EPS)
        for t in range(chips):
            piece = x[part, t * half:(t + 1) * half].astype(jnp.float32)
            piece = piece * inv * gain[:, t * half:(t + 1) * half]
            xs[t, part, :] = piece.astype(jnp.bfloat16)
        if c == 0:
            near = jnp.minimum(i, reach) + jnp.minimum(s - 1 - i, reach)
            pl.semaphore_wait(barrier, chips + near)
        for o in range(1, chips):
            xsendcopy(o, c).start()
        if c == 0:
            wsend().start()
            wcopy.start()
            bcopy.start()
            qcopy.start()

    first = i * tokens
    width = reach * tokens + QB
    for u in range(tokens // QB):
        pos = first + u * QB + lax.broadcasted_iota(jnp.int32, (QB, 1), 0)
        start = jnp.zeros((QB, 1), jnp.int32)
        end = jnp.int32(0)
        for d in range(docs.shape[1]):
            end = end + docs[0, d]
            start = jnp.where(pos >= end, end, start)
        key = first + u * QB - reach * tokens + lax.broadcasted_iota(jnp.int32, (QB, width), 1)
        mask[u] = jnp.where((key >= start) & (key <= pos), 0.0, MASKED)
    for b in range(1, reach + 1):
        @pl.when(i < b)
        def _():
            kv[:, (reach - b) * tokens:(reach - b + 1) * tokens, :] = jnp.zeros(
                (MSGS, tokens, HD), jnp.bfloat16
            )

    def project(left, j, kind):
        cols = pl.ds(pl.multiple_of(kind * (KVH * HD) + j * PAIR, PAIR), PAIR)
        total = jnp.dot(left[:, :rows], w[0, :, cols], preferred_element_type=jnp.float32)
        return total + jnp.dot(
            left[:, rows:], w[1, :, cols], preferred_element_type=jnp.float32
        )

    wcopy.wait()
    wsend().wait()
    bcopy.wait()
    qcopy.wait()

    @pl.loop(0, PAIRS)
    def _(j):
        keys = project(xs.at[chip], j, 0)
        values = project(xs.at[chip], j, 1)
        values = values + vbias[:, pl.ds(pl.multiple_of(j * PAIR, PAIR), PAIR)]
        for h in range(2):
            own[4 * j + 2 * h] = keys[:, h * HD:(h + 1) * HD]
            own[4 * j + 2 * h + 1] = values[:, h * HD:(h + 1) * HD]

    def psendcopy(o, m, part):
        source = lax.rem(chip + chips - o, chips)
        return pltpu.make_async_remote_copy(
            ps.at[o - 1, m, part], pr.at[o - 1, m, part], psend.at[o - 1, m], precv.at[o - 1, m],
            device_id={"fsdp": source * 2 + core},
        )

    whole = pl.ds(0, tokens)

    def give_back(o, j, part):
        for kind in range(2):
            partial = project(xr.at[o - 1, part], j, kind).astype(jnp.bfloat16)
            for h in range(2):
                ps[o - 1, 4 * j + 2 * h + kind, part, :] = partial[:, h * HD:(h + 1) * HD]
        for m in range(4):
            psendcopy(o, 4 * j + m, part).start()

    ahead = XCH - 2
    early = pl.ds(0, ahead * step)
    late = pl.ds(ahead * step, tokens - ahead * step)
    for o in range(1, chips):
        for c in range(ahead):
            xsendcopy(o, c).wait_recv()
        give_back(o, 0, early)
    for o in range(1, chips):
        for c in range(ahead, XCH):
            xsendcopy(o, c).wait_recv()
        give_back(o, 0, late)

    @pl.loop(1, PAIRS)
    def _(j):
        for o in range(1, chips):
            give_back(o, j, whole)

    def slot(b):
        return pl.ds((reach - b) * tokens, tokens)

    def shiftcopy(b, m):
        return pltpu.make_async_remote_copy(
            kv.at[m, slot(0)], kv.at[m, slot(b)], ssend.at[b - 1, m], srecv.at[b - 1, m],
            device_id={"sp": i + b},
        )

    def relay(m):
        return pltpu.make_async_remote_copy(
            kv.at[m, slot(2)], kv.at[m, slot(1)], fsend.at[m], srecv.at[0, m],
            device_id={"sp": i - 1},
        )

    odd = lax.rem(i, 2) == 1

    def sends(b):
        return (i + b < s) & jnp.logical_not(odd) if b == 1 else i + b < s

    def finish(m):
        total = own[m]
        for o in range(1, chips):
            psendcopy(o, m, whole).wait_recv()
            total = total + pr[o - 1, m].astype(jnp.float32)
        kv[m, reach * tokens:, :] = total.astype(jnp.bfloat16)
        for b in range(reach, 0, -1):
            @pl.when(sends(b))
            def _():
                shiftcopy(b, m).start()

    def pass_on(m):
        @pl.when(i >= 2)
        def _():
            shiftcopy(2, m).wait_recv()

        @pl.when(odd & (i >= 3))
        def _():
            relay(m).start()

    def arrive(m):
        for b in range(1, reach + 1):
            if b != 2:
                @pl.when(i >= b)
                def _():
                    shiftcopy(b, m).wait_recv()

    factor = HD ** (-0.5) * math.log2(math.e)
    ratio = QH // KVH

    def attend(g):
        base = pl.multiple_of(g * ratio * HD, HD)
        for u in range(tokens // QB):
            left = jnp.concatenate(
                [q[u * QB:(u + 1) * QB, pl.ds(base + r * HD, HD)] for r in range(ratio)], 0
            )
            keys = kv[2 * g, u * QB:u * QB + width, :]
            values = kv[2 * g + 1, u * QB:u * QB + width, :]
            scores = lax.dot_general(
                left, keys, (((1,), (1,)), ((), ())), preferred_element_type=jnp.float32
            )
            scores = scores.reshape(ratio, QB, width) + mask[u][None]
            scores = scores.reshape(ratio * QB, width)
            highest = jnp.max(scores, axis=-1, keepdims=True)
            probs = jnp.exp2((scores - highest) * factor)
            total = jnp.sum(probs, axis=-1, keepdims=True)
            result = jnp.dot(
                probs.astype(jnp.bfloat16), values, preferred_element_type=jnp.float32
            )
            result = (result / total).astype(jnp.bfloat16)
            for r in range(ratio):
                out[u * QB:(u + 1) * QB, pl.ds(base + r * HD, HD)] = result[
                    r * QB:(r + 1) * QB
                ]

    @pl.loop(0, KVH + 2)
    def _(t):
        for kind in range(2):
            @pl.when(t < KVH)
            def _():
                finish(2 * t + kind)

            @pl.when((t >= 1) & (t < KVH + 1))
            def _():
                pass_on(2 * t - 2 + kind)

        @pl.when(t >= 2)
        def _():
            arrive(2 * t - 4)
            arrive(2 * t - 3)
            attend(t - 2)

    for o in range(1, chips):
        for c in range(XCH):
            xsendcopy(o, c).wait_send()

    @pl.loop(0, MSGS)
    def _(m):
        for o in range(1, chips):
            psendcopy(o, m, whole).wait_send()
        for b in range(1, reach + 1):
            @pl.when(sends(b))
            def _():
                shiftcopy(b, m).wait_send()

        @pl.when(odd & (i >= 3))
        def _():
            relay(m).wait_send()


def shards(n, s, hidden, queries, norm_gain, kv_weight, value_bias, doc_lengths):
    _, tokens, depth = hidden.shape
    reach = s // 4
    chips = n // 2
    rows = kv_weight.shape[0]
    far = chips - 1
    vmem = pltpu.VMEM
    dma = pltpu.SemaphoreType.DMA
    anywhere = pl.BlockSpec(memory_space=pltpu.HBM)
    result = pl.pallas_call(
        functools.partial(kernel, n, s, reach),
        out_shape=jax.ShapeDtypeStruct((tokens, QH * HD), jnp.bfloat16),
        in_specs=[anywhere] * 5 + [pl.BlockSpec(memory_space=pltpu.SMEM)],
        out_specs=pl.BlockSpec(memory_space=pltpu.VMEM),
        scratch_shapes=[
            vmem((tokens, depth), jnp.bfloat16),
            vmem((tokens, QH * HD), jnp.bfloat16),
            vmem((1, depth), jnp.float32),
            vmem((1, KVH * HD), jnp.float32),
            vmem((2, rows, 2 * KVH * HD), jnp.bfloat16),
            vmem((chips, tokens, 2 * rows), jnp.bfloat16),
            vmem((far, tokens, 2 * rows), jnp.bfloat16),
            vmem((MSGS, tokens, HD), jnp.float32),
            vmem((far, MSGS, tokens, HD), jnp.bfloat16),
            vmem((far, MSGS, tokens, HD), jnp.bfloat16),
            vmem((MSGS, (reach + 1) * tokens, HD), jnp.bfloat16),
            vmem((tokens // QB, QB, reach * tokens + QB), jnp.float32),
            dma((4,)),
            dma((XCH,)),
            dma((2,)),
            dma((far, XCH)),
            dma((far, XCH)),
            dma((far, MSGS)),
            dma((far, MSGS)),
            dma((reach, MSGS)),
            dma((reach, MSGS)),
            dma((MSGS,)),
        ],
        compiler_params=pltpu.CompilerParams(
            collective_id=0, has_side_effects=True, vmem_limit_bytes=50 * 1024 * 1024
        ),
    )(
        hidden[0], queries[0], norm_gain.reshape(1, depth), kv_weight,
        value_bias.reshape(1, KVH * HD), doc_lengths,
    )
    return result.reshape(1, tokens, QH * HD)


def solution(mesh):
    in_specs = (
        P("fsdp", "sp", None),
        P("fsdp", "sp", None),
        P(),
        P("fsdp", None),
        P(),
        P("fsdp", None),
    )
    body = functools.partial(shards, mesh.shape["fsdp"], mesh.shape["sp"])
    return jax.shard_map(
        body, mesh=mesh, in_specs=in_specs, out_specs=P("fsdp", "sp", None), check_vma=False
    )
```
